32 devices in a mesh: section: 8 (over z, core), expert: 4 (over y, x).
Axes of the slice: x: 2, y: 2, z: 4, core: 2. Of those that a mesh axis runs over, the one named last changes fastest.
Arguments:
- state: bfloat16 [8, 512, 2048], P('section', 'expert'), may hold values from -6 to 6
- norm_gain: float32 [8, 2048], P('section'), may hold values from 0.25 to 1.75
- expert_in: bfloat16 [8, 4, 2048, 1536], P('section', 'expert'), may hold values from -0.125 to 0.125
- expert_out: bfloat16 [8, 4, 768, 2048], P('section', 'expert'), may hold values from -0.21875 to 0.21875
- route_ids: int32 [3, 8, 512, 6], P(None, 'section', 'expert'), may hold values from 0 to 63, all different within a row
- route_weights: float32 [3, 8, 512, 6], P(None, 'section', 'expert'), may hold values from 0.3 to 3
Outputs:
- state_out: bfloat16 [8, 512, 2048], P('section', 'expert')
The draws below stay inside these ranges and needn't reach their ends.
Inputs may be any that keep to these rules, and one draw needn't show every extreme that they name: `route_ids`: each token names 6 different experts.
All inputs are finite; a program needn't handle non-finite values.
Results may differ from the reference program's by a relative error of at most 0.02.
Values may be sent and summed in bfloat16 or wider, within the bound.
A program may use at most 64 MiB of HBM per device.

```python
import math
from functools import partial
import jax
import jax.numpy as jnp
from jax import lax

D = 2048
ROUTED = 64
TOP = 6
FF = 768
TICKS = 3
TOK_DEV = 128
CAP = 32
EXPERTS = 4
TOKENS = 512
N_SECTION = 8
N_EXPERT = 4


def steps_of(stream_key, extent, pieces, least, high):
    gain, own = 1.0, jax.random.fold_in(stream_key, 6)
    for position, parts in pieces:
        draws = jnp.exp(jax.random.uniform(jax.random.fold_in(own, position), (parts,), jnp.float32, least / len(pieces), high / len(pieces)))
        gain = gain * jnp.repeat(draws, extent[position] // parts).reshape([-1 if axis == position else 1 for axis in range(len(extent))])
    return gain


def choose_distinct(rng, rows, count, top, lift):
    ranking = jax.random.permutation(jax.random.fold_in(rng, 1), count)
    boost = ranking
    for power in range(3):
        boost = boost * boost // count
    boost = boost * lift // count
    lots = jax.random.randint(jax.random.fold_in(rng, 2), (rows, count), 0, 4096) + boost
    fixed_rows = jax.random.permutation(jax.random.fold_in(rng, 3), rows)[jnp.arange(count) % rows]
    lots = jnp.where(jnp.arange(rows)[:, None] == fixed_rows[None, :], 1 << 14, lots)
    priority = lots * count + jnp.arange(count)
    return lax.top_k(priority.astype(jnp.int32), top)[1].astype(jnp.int32)


def noise(stream_key, extent, deviation, most, pieces=(), kind=jnp.bfloat16):
    gain = steps_of(stream_key, extent, pieces, -0.22, 0.18) if pieces else 1.0
    result = jax.random.normal(stream_key, extent, jnp.float32) * deviation * gain
    return jnp.minimum(jnp.maximum(result, -most), most).astype(kind)


def setup_inputs(seed: int = 0) -> dict:
    splits = jax.random.split(jax.random.key(seed), 7)
    state = noise(splits[0], (N_SECTION, TOKENS, D), 1.0, 6.0, ((0, 8), (1, 4)))
    norm_gain = jnp.clip(1.0 + 0.15 * jax.random.normal(splits[1], (N_SECTION, D), jnp.float32), 0.25, 1.75)
    expert_in = noise(splits[2], (N_SECTION, EXPERTS, D, 2 * FF), D ** -0.5, 0.125, ((0, 8), (1, 4)))
    expert_out = noise(splits[3], (N_SECTION, EXPERTS, FF, D), FF ** -0.5, 0.21875, ((0, 8), (1, 4)))
    route_ids = choose_distinct(splits[4], TICKS * N_SECTION * TOKENS, ROUTED, TOP, 1536).reshape((TICKS, N_SECTION, TOKENS, TOP))
    route_weights = jnp.clip(jnp.exp(math.log(3.0) - 2.3025851 * jax.random.uniform(splits[5], (TICKS, N_SECTION, TOKENS, TOP), jnp.float32) ** steps_of(splits[5], (TICKS, N_SECTION, TOKENS, TOP), ((1, 8), (2, 4)), -0.2, 0.2)), 0.3, 3.0)
    return dict(state=state, norm_gain=norm_gain, expert_in=expert_in, expert_out=expert_out, route_ids=route_ids, route_weights=route_weights)


epsilon = 1e-06

def normalize(hidden, gain_row):
    widened = hidden.astype(jnp.float32)
    rescale = lax.rsqrt(lax.optimization_barrier(jnp.mean(widened * widened, axis=-1, keepdims=True)) + epsilon)
    return (widened * rescale * gain_row).astype(jnp.bfloat16)

def slot_tables(chosen, experts, capacity):
    window = jnp.arange(experts, dtype=jnp.int32)
    choice_hits = (chosen[:, :, None] == window[None, None, :]).astype(jnp.int32)
    picked = lax.optimization_barrier(jnp.sum(choice_hits, axis=1))
    rank_table = jnp.cumsum(picked, axis=0) - picked
    kept_table = picked * (rank_table < capacity).astype(jnp.int32)
    slot_index = jnp.arange(capacity, dtype=jnp.int32)
    slot_match = kept_table[:, :, None] * (rank_table[:, :, None] == slot_index[None, None, :]).astype(jnp.int32)
    positions = jnp.arange(chosen.shape[0], dtype=jnp.int32)
    token_at = lax.optimization_barrier(jnp.sum(slot_match * positions[:, None, None], axis=0))
    filled = lax.optimization_barrier(jnp.sum(slot_match, axis=0))
    kept_hits = choice_hits * kept_table[:, None, :]
    kept_choice = lax.optimization_barrier(jnp.sum(kept_hits, axis=2))
    flat_slot = lax.optimization_barrier(jnp.sum(kept_hits * (window[None, None, :] * capacity + rank_table[:, None, :]), axis=2))
    return (token_at, filled, flat_slot, kept_choice)

def expert_forward(token_rows, inner_weight, outer_weight):
    projected = jnp.dot(token_rows, inner_weight, preferred_element_type=jnp.float32)
    hidden_units = outer_weight.shape[0]
    activated = (jax.nn.silu(projected[:, :hidden_units]) * projected[:, hidden_units:]).astype(jnp.bfloat16)
    return jnp.dot(activated, outer_weight, preferred_element_type=jnp.float32).astype(jnp.bfloat16)

def serve_expert(operands):
    arrived, inner_one, outer_one = operands
    token_rows = arrived.reshape(-1, arrived.shape[-1])
    return expert_forward(token_rows, inner_one, outer_one).reshape(arrived.shape)

def layer(operands):
    hidden, gain_row, inner_weight, outer_weight, chosen, weights = operands
    normed = normalize(hidden, gain_row).reshape(N_EXPERT, TOK_DEV, D)
    tables = jax.vmap(partial(slot_tables, experts=EXPERTS, capacity=CAP))
    token_at, filled, flat_slot, kept_choice = tables(chosen.reshape(N_EXPERT, TOK_DEV, TOP))
    taker = jax.vmap(partial(jnp.take, axis=0))
    outbound = taker(normed, token_at) * filled[:, :, :, None].astype(jnp.bfloat16)
    served = lax.map(serve_expert, (jnp.swapaxes(outbound, 0, 1), inner_weight, outer_weight))
    returned = jnp.swapaxes(served, 0, 1).reshape(N_EXPERT, EXPERTS * CAP, D)
    picked_rows = taker(returned, flat_slot)
    mixing = weights.reshape(N_EXPERT, TOK_DEV, TOP) * kept_choice.astype(weights.dtype)
    branch = jnp.einsum('btk,btkd->btd', mixing, picked_rows.astype(jnp.float32))
    return (hidden.astype(jnp.float32) + branch.reshape(TOKENS, D)).astype(jnp.bfloat16)

def reference(state, norm_gain, expert_in, expert_out, route_ids, route_weights):
    holding = state
    for tick_index in range(TICKS):
        moved = lax.map(layer, (holding, norm_gain, expert_in, expert_out, route_ids[tick_index], route_weights[tick_index]))
        holding = jnp.roll(moved, 1, axis=0)
    return holding
```

```python
import functools

import jax
import jax.numpy as jnp
from jax import lax
from jax.experimental import pallas as pl
from jax.experimental.pallas import tpu as pltpu
from jax.sharding import PartitionSpec as P

epsilon = 1e-06
COLUMN_SHARES = (1, 1, 1, 1)
SLOT_SHARES = (1, 1)
MESH = pl.DeviceIdType.MESH


def cuts(total, shares):
    whole = sum(shares)
    ends = [total * sum(shares[: i + 1]) // whole for i in range(len(shares))]
    starts = [0] + ends[:-1]
    return [(a, b - a) for a, b in zip(starts, ends)]


def relay_kernel(
    sections,
    experts,
    state_hbm,
    gain_hbm,
    win_hbm,
    wout_hbm,
    ids_hbm,
    wts_hbm,
    out_ref,
    win,
    wout,
    gain,
    ids,
    wts,
    ids_before,
    wts_before,
    state,
    hcur,
    arrive,
    first,
    pick,
    comb,
    sendbuf,
    recvbuf,
    retsend,
    acc,
    load_sem,
    win_sem,
    state_sem,
    route_ss,
    route_rs,
    disp_ss,
    disp_rs,
    ret_ss,
    ret_rs,
    h_ss,
    h_rs,
):
    ticks, top = ids.shape[:2]
    tokens = state[0].shape[0]
    columns = cuts(state_hbm.shape[2], COLUMN_SHARES)
    width = state_hbm.shape[2]
    chunks = len(columns)
    hidden_units = wout.shape[0]
    capacity = tokens // 4
    slots = experts * capacity
    parts = cuts(capacity, SLOT_SHARES)

    section = lax.axis_index("section")
    me = lax.axis_index("expert")
    after = lax.rem(section + 1, sections)
    before = lax.rem(section + sections - 1, sections)
    others = range(1, experts)

    barrier = pltpu.get_barrier_semaphore()
    for d in others:
        pl.semaphore_signal(
            barrier,
            inc=1,
            device_id={"section": section, "expert": lax.rem(me + d, experts)},
            device_id_type=MESH,
        )
    for e in range(experts):
        pl.semaphore_signal(
            barrier, inc=1, device_id={"section": before, "expert": e}, device_id_type=MESH
        )

    load_ids = pltpu.make_async_copy(ids_hbm, ids, load_sem.at[0])
    load_wts = pltpu.make_async_copy(wts_hbm, wts, load_sem.at[1])
    load_gain = pltpu.make_async_copy(gain_hbm, gain, load_sem.at[2])
    load_out = pltpu.make_async_copy(wout_hbm.at[0, 0], wout, load_sem.at[3])

    def load_state(c):
        start, size = columns[c]
        return pltpu.make_async_copy(
            state_hbm.at[0, :, pl.ds(start, size)], state[c], state_sem.at[c]
        )

    def load_in(c):
        rows = pl.ds(*columns[c])
        return pltpu.make_async_copy(win_hbm.at[0, 0, rows], win.at[rows], win_sem.at[c])

    load_ids.start()
    for c in range(chunks):
        load_state(c).start()
    load_wts.start()
    load_gain.start()
    for c in range(chunks):
        load_in(c).start()
    load_out.start()

    slot_row = lax.broadcasted_iota(jnp.int32, (slots, tokens), 0)
    expert_of = jnp.zeros((slots, tokens), jnp.int32)
    slot_of = slot_row
    for low, half in parts:
        for e in range(experts):
            start = low * experts + e * half
            inside = slot_row >= start
            expert_of = jnp.where(inside, e, expert_of)
            slot_of = jnp.where(inside, slot_row - start + low, slot_of)
    slot_of = slot_of.astype(jnp.float32)
    row_i = lax.broadcasted_iota(jnp.int32, (tokens, tokens), 0)
    col_i = lax.broadcasted_iota(jnp.int32, (tokens, tokens), 1)
    earlier = jnp.where(row_i < col_i, 1.0, 0.0).astype(jnp.bfloat16)

    def kept_slots(ids_ref, t):
        hit = jnp.zeros((slots, tokens), jnp.float32)
        for k in range(top):
            hit = jnp.where(ids_ref[t, k] == expert_of, 1.0, hit)
        rank = jnp.dot(hit.astype(jnp.bfloat16), earlier, preferred_element_type=jnp.float32)
        return jnp.where(rank == slot_of, hit, 0.0)

    def make_comb(t):
        mix = jnp.zeros((slots, tokens), jnp.float32)
        for k in range(top):
            mix = jnp.where(ids_before[t, k] == expert_of, wts_before[t, k], mix)
        weighted = kept_slots(ids_before, t) * mix
        comb[t] = jnp.transpose(weighted).astype(jnp.bfloat16)

    def make_pick(t):
        keep = kept_slots(ids, t).astype(jnp.bfloat16)
        mixed = jnp.dot(keep, comb[t - 1], preferred_element_type=jnp.float32)
        pick[t - 1, :, pl.ds(0, slots)] = mixed.astype(jnp.bfloat16)
        pick[t - 1, :, pl.ds(slots, tokens)] = keep

    def route_copies():
        return [
            pltpu.make_async_remote_copy(
                src_ref=mine,
                dst_ref=theirs,
                send_sem=route_ss.at[i],
                recv_sem=route_rs.at[i],
                device_id={"section": after, "expert": me},
                device_id_type=MESH,
            )
            for i, (mine, theirs) in enumerate(((ids, ids_before), (wts, wts_before)))
        ]

    def h_copy(t, c):
        return pltpu.make_async_remote_copy(
            src_ref=state[c] if t == 0 else hcur[c].at[t - 1],
            dst_ref=arrive[c].at[t, pl.ds(slots, tokens)],
            send_sem=h_ss.at[t, c],
            recv_sem=h_rs.at[t, c],
            device_id={"section": after, "expert": me},
            device_id_type=MESH,
        )

    def part_rows(p, e):
        low, half = parts[p]
        return pl.ds(pl.multiple_of(low * experts + e * half, 8), half)

    def part_all(p):
        low, half = parts[p]
        return pl.ds(low * experts, half * experts)

    def send_rows(t, p, c):
        for d in others:
            peer = lax.rem(me + d, experts)
            pltpu.make_async_remote_copy(
                src_ref=sendbuf[c].at[t, part_rows(p, peer)],
                dst_ref=recvbuf[c].at[t, part_rows(p, me)],
                send_sem=disp_ss.at[t, c],
                recv_sem=disp_rs.at[t, p, c],
                device_id={"section": section, "expert": peer},
                device_id_type=MESH,
            ).start()

    def await_rows(t, p, c):
        low, half = parts[p]
        block = recvbuf[c].at[t, pl.ds(low * experts, (experts - 1) * half)]
        pltpu.make_async_remote_copy(
            src_ref=block,
            dst_ref=block,
            send_sem=disp_ss.at[t, c],
            recv_sem=disp_rs.at[t, p, c],
            device_id={"section": section, "expert": lax.rem(me + 1, experts)},
            device_id_type=MESH,
        ).wait_recv()

    def send_served(t, p, c):
        for d in (*others, 0):
            peer = lax.rem(me + d, experts)
            pltpu.make_async_remote_copy(
                src_ref=retsend[c].at[t, part_rows(p, peer)],
                dst_ref=arrive[c].at[t, part_rows(p, me)],
                send_sem=ret_ss.at[t, c],
                recv_sem=ret_rs.at[t, c],
                device_id={"section": after, "expert": peer},
                device_id_type=MESH,
            ).start()

    def served_copy(t, c):
        return pltpu.make_async_remote_copy(
            src_ref=retsend[c].at[t],
            dst_ref=arrive[c].at[t, pl.ds(0, slots)],
            send_sem=ret_ss.at[t, c],
            recv_sem=ret_rs.at[t, c],
            device_id={"section": before, "expert": me},
            device_id_type=MESH,
        )

    def fill(t, c, picker, source):
        rows = jnp.dot(picker, source, preferred_element_type=jnp.float32)
        sendbuf[c][t] = rows.astype(jnp.bfloat16)

    def keep_own(t, c):
        for p in range(len(parts)):
            own = part_rows(p, me)
            recvbuf[c][t, own, :] = sendbuf[c][t, own, :]

    def dispatch(t, c):
        send_rows(t, 0, c)
        if c == chunks - 1:
            for p in range(1, len(parts)):
                for late in range(chunks):
                    send_rows(t, p, late)

    load_ids.wait()
    first[...] = kept_slots(ids, 0).astype(jnp.bfloat16)
    for c in range(chunks):
        load_state(c).wait()
        fill(0, c, first[...], state[c][...])
        keep_own(0, c)
    load_wts.wait()
    pl.semaphore_wait(barrier, experts - 1 + experts)
    for c in range(chunks):
        dispatch(0, c)
    for copy in route_copies():
        copy.start()
    for c in range(chunks):
        h_copy(0, c).start()
    for copy in route_copies():
        copy.wait_recv()
    for t in range(ticks):
        make_comb(t)
    for t in range(1, ticks):
        make_pick(t)

    load_gain.wait()
    for t in range(ticks):
        for p in range(len(parts)):
            rows = part_all(p)
            group = rows.size
            squares = jnp.zeros((group, 1), jnp.float32)
            for c in range(chunks):
                cols = pl.ds(*columns[c])
                if t == 0 and p == 0:
                    load_in(c).wait()
                await_rows(t, p, c)
                wide = recvbuf[c][t, rows, :].astype(jnp.float32)
                squares = squares + jnp.sum(wide * wide, axis=-1, keepdims=True)
                scaled = (wide * gain[:, cols]).astype(jnp.bfloat16)
                part = jnp.dot(scaled, win[cols, :], preferred_element_type=jnp.float32)
                if c == 0:
                    acc[pl.ds(0, group), :] = part
                else:
                    acc[pl.ds(0, group), :] += part
            rescale = lax.rsqrt(squares / width + epsilon)
            gate = acc[pl.ds(0, group), :hidden_units] * rescale
            up = acc[pl.ds(0, group), hidden_units:] * rescale
            activated = (gate / (1.0 + jnp.exp(-gate)) * up).astype(jnp.bfloat16)
            if t == 0 and p == 0:
                load_out.wait()
            for c in range(chunks):
                served = jnp.dot(
                    activated, wout[:, pl.ds(*columns[c])], preferred_element_type=jnp.float32
                )
                retsend[c][t, rows, :] = served.astype(jnp.bfloat16)
                send_served(t, p, c)
        for c in range(chunks):
            h_copy(t, c).wait_recv()
            served_copy(t, c).wait_recv()
            if t < ticks - 1:
                fill(t + 1, c, pick[t], arrive[c][t])
                dispatch(t + 1, c)
            branch = jnp.dot(
                comb[t], arrive[c][t, pl.ds(0, slots)], preferred_element_type=jnp.float32
            )
            stay = arrive[c][t, pl.ds(slots, tokens)].astype(jnp.float32)
            fresh = (stay + branch).astype(jnp.bfloat16)
            if t == ticks - 1:
                out_ref[0, :, pl.ds(*columns[c])] = fresh
            else:
                hcur[c][t] = fresh
                h_copy(t + 1, c).start()
                keep_own(t + 1, c)

    for copy in route_copies():
        copy.wait_send()
    for t in range(ticks):
        for c in range(chunks):
            h_copy(t, c).wait_send()
            sent = sendbuf[c].at[t, pl.ds(0, slots - capacity)]
            pltpu.make_async_remote_copy(
                src_ref=sent,
                dst_ref=sent,
                send_sem=disp_ss.at[t, c],
                recv_sem=disp_rs.at[t, 0, c],
                device_id={"section": after, "expert": me},
                device_id_type=MESH,
            ).wait_send()
            served_copy(t, c).wait_send()


def on_device(sections, experts, state, norm_gain, expert_in, expert_out, route_ids, route_weights):
    ticks, _, _, top = route_ids.shape
    tokens, width = state.shape[1:]
    inner = expert_in.shape[3]
    hidden_units = expert_out.shape[2]
    slots = experts * (tokens // 4)
    columns = cuts(width, COLUMN_SHARES)
    chunks, parts = len(columns), len(SLOT_SHARES)
    widest = max(size for _, size in cuts(tokens // 4, SLOT_SHARES)) * experts
    bf16 = jnp.bfloat16
    hbm = pl.BlockSpec(memory_space=pltpu.HBM)
    dma = pltpu.SemaphoreType.DMA

    def per_chunk(*shape):
        return [pltpu.VMEM((*shape, size), bf16) for _, size in columns]

    def in_hbm(x):
        return pltpu.with_memory_space_constraint(x, pltpu.HBM)

    return pl.pallas_call(
        functools.partial(relay_kernel, sections, experts),
        out_shape=pltpu.VMEM(state.shape, state.dtype),
        in_specs=[hbm] * 6,
        out_specs=pl.BlockSpec(memory_space=pltpu.VMEM),
        scratch_shapes=[
            pltpu.VMEM((width, inner), bf16),
            pltpu.VMEM((hidden_units, width), bf16),
            pltpu.VMEM((1, width), jnp.float32),
            pltpu.VMEM((ticks, top, 1, tokens), jnp.int32),
            pltpu.VMEM((ticks, top, 1, tokens), jnp.float32),
            pltpu.VMEM((ticks, top, 1, tokens), jnp.int32),
            pltpu.VMEM((ticks, top, 1, tokens), jnp.float32),
            per_chunk(tokens),
            per_chunk(max(ticks - 1, 1), tokens),
            per_chunk(ticks, slots + tokens),
            pltpu.VMEM((slots, tokens), bf16),
            pltpu.VMEM((max(ticks - 1, 1), slots, slots + tokens), bf16),
            pltpu.VMEM((ticks, tokens, slots), bf16),
            per_chunk(ticks, slots),
            per_chunk(ticks, slots),
            per_chunk(ticks, slots),
            pltpu.VMEM((widest, inner), jnp.float32),
            dma((4,)),
            dma((chunks,)),
            dma((chunks,)),
            dma((2,)),
            dma((2,)),
            dma((ticks, chunks)),
            dma((ticks, parts, chunks)),
            dma((ticks, chunks)),
            dma((ticks, chunks)),
            dma((ticks, chunks)),
            dma((ticks, chunks)),
        ],
        compiler_params=pltpu.CompilerParams(
            collective_id=0, has_side_effects=True, vmem_limit_bytes=48 * 2**20
        ),
        name="relay",
    )(
        in_hbm(state),
        in_hbm(norm_gain),
        in_hbm(expert_in),
        in_hbm(expert_out),
        in_hbm(jnp.transpose(route_ids, (0, 3, 1, 2))),
        in_hbm(jnp.transpose(route_weights, (0, 3, 1, 2))),
    )


def solution(mesh):
    in_specs = (
        P("section", "expert", None),
        P("section", None),
        P("section", "expert", None, None),
        P("section", "expert", None, None),
        P(None, "section", "expert", None),
        P(None, "section", "expert", None),
    )
    out_specs = P("section", "expert", None)
    return jax.shard_map(
        functools.partial(on_device, mesh.shape["section"], mesh.shape["expert"]),
        mesh=mesh,
        in_specs=in_specs,
        out_specs=out_specs,
        check_vma=False,
    )
```

```python
import functools

import jax
import jax.numpy as jnp
from jax import lax
from jax.experimental import pallas as pl
from jax.experimental.pallas import tpu as pltpu
from jax.sharding import PartitionSpec as P

epsilon = 1e-06
COLUMN_SHARES = (1, 1, 1, 1)
SLOT_SHARES = (1, 1)
DISPATCH_RUNS = ((1, 1, 1, 1), (1, 1, 1, 1))
RETURN_RUNS = ((2, 2), (1, 1, 1, 1))
MESH = pl.DeviceIdType.MESH


def cuts(total, shares):
    whole = sum(shares)
    ends = [total * sum(shares[: i + 1]) // whole for i in range(len(shares))]
    starts = [0] + ends[:-1]
    return [(a, b - a) for a, b in zip(starts, ends)]


def runs(lengths):
    ends = [sum(lengths[: i + 1]) for i in range(len(lengths))]
    return [(b - n, b) for b, n in zip(ends, lengths)]


def relay_kernel(
    sections,
    experts,
    state_hbm,
    gain_hbm,
    win_hbm,
    wout_hbm,
    ids_hbm,
    wts_hbm,
    out_ref,
    win,
    wout,
    gain,
    ids,
    wts,
    ids_before,
    wts_before,
    state,
    hcur,
    arrive,
    first,
    pick,
    comb,
    sendbuf,
    recvbuf,
    retsend,
    acc,
    load_sem,
    win_sem,
    state_sem,
    route_ss,
    route_rs,
    disp_ss,
    disp_rs,
    ret_ss,
    ret_rs,
    h_ss,
):
    ticks, top = ids.shape[:2]
    tokens = state.shape[0]
    columns = cuts(state_hbm.shape[2], COLUMN_SHARES)
    width = state_hbm.shape[2]
    chunks = len(columns)
    hidden_units = wout.shape[0]
    capacity = tokens // 4
    slots = experts * capacity
    parts = cuts(capacity, SLOT_SHARES)
    disp_runs = [runs(lengths) for lengths in DISPATCH_RUNS]
    ret_runs = [runs(lengths) for lengths in RETURN_RUNS]

    def disp_sem(p, low):
        return sum(map(len, disp_runs[:p])) + [a for a, _ in disp_runs[p]].index(low)

    def ret_sem(p, low):
        return sum(map(len, ret_runs[:p])) + [a for a, _ in ret_runs[p]].index(low)

    def span(low, high):
        start = columns[low][0]
        return pl.ds(start, sum(columns[high - 1]) - start)

    section = lax.axis_index("section")
    me = lax.axis_index("expert")
    after = lax.rem(section + 1, sections)
    before = lax.rem(section + sections - 1, sections)
    lanes = max(k for k in range(1, experts + 1) if experts % k == 0 and k * k <= experts)
    files = experts // lanes
    steps = [(i, j) for i in range(lanes) for j in range(files)]

    def hops(step):
        i, j = step
        return min(i, lanes - i) + min(j, files - j)

    def peer_at(step):
        i, j = step
        return lax.rem(me // files + i, lanes) * files + lax.rem(lax.rem(me, files) + j, files)

    steps_d = sorted([s for s in steps if s != (0, 0)], key=lambda s: (hops(s), s), reverse=True)
    steps_r = sorted(steps, key=lambda s: (hops(s), s), reverse=True)

    barrier = pltpu.get_barrier_semaphore()
    for step in steps_d:
        pl.semaphore_signal(
            barrier,
            inc=1,
            device_id={"section": section, "expert": peer_at(step)},
            device_id_type=MESH,
        )
    for e in range(experts):
        pl.semaphore_signal(
            barrier, inc=1, device_id={"section": before, "expert": e}, device_id_type=MESH
        )

    load_ids = pltpu.make_async_copy(ids_hbm, ids, load_sem.at[0])
    load_wts = pltpu.make_async_copy(wts_hbm, wts, load_sem.at[1])
    load_gain = pltpu.make_async_copy(gain_hbm, gain, load_sem.at[2])
    load_out = pltpu.make_async_copy(wout_hbm.at[0, 0], wout, load_sem.at[3])

    def load_state(c):
        cols = pl.ds(*columns[c])
        return pltpu.make_async_copy(
            state_hbm.at[0, :, cols], state.at[:, cols], state_sem.at[c]
        )

    def load_in(c):
        rows = pl.ds(*columns[c])
        return pltpu.make_async_copy(win_hbm.at[0, 0, rows], win.at[rows], win_sem.at[c])

    load_ids.start()
    for c in range(chunks):
        load_state(c).start()
    load_wts.start()
    load_gain.start()

    slot_row = lax.broadcasted_iota(jnp.int32, (slots, tokens), 0)
    expert_of = jnp.zeros((slots, tokens), jnp.int32)
    slot_of = slot_row
    for low, half in parts:
        for e in range(experts):
            start = low * experts + e * half
            inside = slot_row >= start
            expert_of = jnp.where(inside, e, expert_of)
            slot_of = jnp.where(inside, slot_row - start + low, slot_of)
    slot_of = slot_of.astype(jnp.float32)
    row_i = lax.broadcasted_iota(jnp.int32, (tokens, tokens), 0)
    col_i = lax.broadcasted_iota(jnp.int32, (tokens, tokens), 1)
    earlier = jnp.where(row_i < col_i, 1.0, 0.0).astype(jnp.bfloat16)

    def kept_slots(ids_ref, t):
        hit = jnp.zeros((slots, tokens), jnp.float32)
        for k in range(top):
            hit = jnp.where(ids_ref[t, k] == expert_of, 1.0, hit)
        rank = jnp.dot(hit.astype(jnp.bfloat16), earlier, preferred_element_type=jnp.float32)
        return jnp.where(rank == slot_of, hit, 0.0)

    def make_comb(t):
        mix = jnp.zeros((slots, tokens), jnp.float32)
        for k in range(top):
            mix = jnp.where(ids_before[t, k] == expert_of, wts_before[t, k], mix)
        weighted = kept_slots(ids_before, t) * mix
        comb[t] = jnp.transpose(weighted).astype(jnp.bfloat16)

    def make_pick(t):
        keep = kept_slots(ids, t).astype(jnp.bfloat16)
        mixed = jnp.dot(keep, comb[t - 1], preferred_element_type=jnp.float32)
        pick[t - 1, :, pl.ds(0, slots)] = mixed.astype(jnp.bfloat16)
        pick[t - 1, :, pl.ds(slots, tokens)] = keep

    def route_copies():
        return [
            pltpu.make_async_remote_copy(
                src_ref=mine,
                dst_ref=theirs,
                send_sem=route_ss.at[i],
                recv_sem=route_rs.at[i],
                device_id={"section": after, "expert": me},
                device_id_type=MESH,
            )
            for i, (mine, theirs) in enumerate(((ids, ids_before), (wts, wts_before)))
        ]

    def h_copy(t, c):
        cols = pl.ds(*columns[c])
        return pltpu.make_async_remote_copy(
            src_ref=state.at[:, cols] if t == 0 else hcur.at[t - 1, :, cols],
            dst_ref=arrive.at[t, pl.ds(slots, tokens), cols],
            send_sem=h_ss,
            recv_sem=ret_rs.at[t, ret_sem(len(parts) - 1, c)],
            device_id={"section": after, "expert": me},
            device_id_type=MESH,
        )

    def part_rows(p, e):
        low, half = parts[p]
        return pl.ds(pl.multiple_of(low * experts + e * half, 8), half)

    def part_all(p):
        low, half = parts[p]
        return pl.ds(low * experts, half * experts)

    def send_rows(t, p, low, high):
        for step in steps_d:
            peer = peer_at(step)
            pltpu.make_async_remote_copy(
                src_ref=sendbuf.at[t, part_rows(p, peer), span(low, high)],
                dst_ref=recvbuf.at[t, part_rows(p, me), span(low, high)],
                send_sem=disp_ss,
                recv_sem=disp_rs.at[t, disp_sem(p, low)],
                device_id={"section": section, "expert": peer},
                device_id_type=MESH,
            ).start()

    def await_rows(t, p, c):
        first_row, half = parts[p]
        for low, high in disp_runs[p]:
            if low == c:
                block = recvbuf.at[
                    t, pl.ds(first_row * experts, (experts - 1) * half), span(low, high)
                ]
                pltpu.make_async_remote_copy(
                    src_ref=block,
                    dst_ref=block,
                    send_sem=disp_ss,
                    recv_sem=disp_rs.at[t, disp_sem(p, low)],
                    device_id={"section": section, "expert": lax.rem(me + 1, experts)},
                    device_id_type=MESH,
                ).wait_recv()

    def send_served(t, p, c):
        for low, high in ret_runs[p]:
            if high == c + 1:
                for step in steps_r:
                    peer = peer_at(step)
                    pltpu.make_async_remote_copy(
                        src_ref=retsend.at[t, part_rows(p, peer), span(low, high)],
                        dst_ref=arrive.at[t, part_rows(p, me), span(low, high)],
                        send_sem=ret_ss,
                        recv_sem=ret_rs.at[t, ret_sem(p, low)],
                        device_id={"section": after, "expert": peer},
                        device_id_type=MESH,
                    ).start()

    def await_served(t, c):
        last = len(parts) - 1
        for p in range(len(parts)):
            for low, high in ret_runs[p]:
                if low == c:
                    rows = part_all(p)
                    if p == last:
                        rows = pl.ds(rows.start, rows.size + tokens)
                    block = arrive.at[t, rows, span(low, high)]
                    pltpu.make_async_remote_copy(
                        src_ref=block,
                        dst_ref=block,
                        send_sem=ret_ss,
                        recv_sem=ret_rs.at[t, ret_sem(p, low)],
                        device_id={"section": before, "expert": me},
                        device_id_type=MESH,
                    ).wait_recv()

    def fill(t, c, picker, source):
        rows = jnp.dot(picker, source, preferred_element_type=jnp.float32)
        sendbuf[t, :, pl.ds(*columns[c])] = rows.astype(jnp.bfloat16)

    def keep_own(t, c):
        cols = pl.ds(*columns[c])
        for p in range(len(parts)):
            own = part_rows(p, me)
            recvbuf[t, own, cols] = sendbuf[t, own, cols]

    def dispatch(t, c):
        for low, high in disp_runs[0]:
            if high == c + 1:
                send_rows(t, 0, low, high)
        if c == chunks - 1:
            for p in range(1, len(parts)):
                for low, high in disp_runs[p]:
                    send_rows(t, p, low, high)

    load_ids.wait()
    first[...] = kept_slots(ids, 0).astype(jnp.bfloat16)
    for c in range(chunks):
        load_state(c).wait()
        fill(0, c, first[...], state[:, pl.ds(*columns[c])])
        keep_own(0, c)
    for c in range(chunks):
        load_in(c).start()
    load_out.start()
    load_wts.wait()
    pl.semaphore_wait(barrier, experts - 1 + experts)
    for copy in route_copies():
        copy.start()
    for c in range(chunks):
        dispatch(0, c)
    for c in range(chunks):
        h_copy(0, c).start()
    for copy in route_copies():
        copy.wait_recv()
    for t in range(ticks):
        make_comb(t)
    for t in range(1, ticks):
        make_pick(t)

    load_gain.wait()
    for t in range(ticks):
        for p in range(len(parts)):
            rows = part_all(p)
            group = rows.size
            squares = jnp.zeros((group, 1), jnp.float32)
            for c in range(chunks):
                cols = pl.ds(*columns[c])
                if t == 0 and p == 0:
                    load_in(c).wait()
                await_rows(t, p, c)
                wide = recvbuf[t, rows, cols].astype(jnp.float32)
                squares = squares + jnp.sum(wide * wide, axis=-1, keepdims=True)
                scaled = (wide * gain[:, cols]).astype(jnp.bfloat16)
                part = jnp.dot(scaled, win[cols, :], preferred_element_type=jnp.float32)
                if c == 0:
                    acc[pl.ds(0, group), :] = part
                else:
                    acc[pl.ds(0, group), :] += part
            rescale = lax.rsqrt(squares / width + epsilon)
            gate = acc[pl.ds(0, group), :hidden_units] * rescale
            up = acc[pl.ds(0, group), hidden_units:] * rescale
            activated = (gate / (1.0 + jnp.exp(-gate)) * up).astype(jnp.bfloat16)
            if t == 0 and p == 0:
                load_out.wait()
            for c in range(chunks):
                served = jnp.dot(
                    activated, wout[:, pl.ds(*columns[c])], preferred_element_type=jnp.float32
                )
                retsend[t, rows, pl.ds(*columns[c])] = served.astype(jnp.bfloat16)
                send_served(t, p, c)
        for c in range(chunks):
            cols = pl.ds(*columns[c])
            await_served(t, c)
            if t < ticks - 1:
                fill(t + 1, c, pick[t], arrive[t, :, cols])
                dispatch(t + 1, c)
            branch = jnp.dot(
                comb[t], arrive[t, pl.ds(0, slots), cols], preferred_element_type=jnp.float32
            )
            stay = arrive[t, pl.ds(slots, tokens), cols].astype(jnp.float32)
            fresh = (stay + branch).astype(jnp.bfloat16)
            if t == ticks - 1:
                out_ref[0, :, cols] = fresh
            else:
                hcur[t, :, cols] = fresh
                h_copy(t + 1, c).start()
                keep_own(t + 1, c)

    for copy in route_copies():
        copy.wait_send()
    for sent, sem in (
        (sendbuf.at[:, pl.ds(0, slots - capacity)], disp_ss),
        (retsend, ret_ss),
        (arrive.at[:, pl.ds(slots, tokens)], h_ss),
    ):
        pltpu.make_async_remote_copy(
            src_ref=sent,
            dst_ref=sent,
            send_sem=sem,
            recv_sem=disp_rs.at[0, 0],
            device_id={"section": after, "expert": me},
            device_id_type=MESH,
        ).wait_send()


def on_device(sections, experts, state, norm_gain, expert_in, expert_out, route_ids, route_weights):
    ticks, _, _, top = route_ids.shape
    tokens, width = state.shape[1:]
    inner = expert_in.shape[3]
    hidden_units = expert_out.shape[2]
    slots = experts * (tokens // 4)
    columns = cuts(width, COLUMN_SHARES)
    chunks = len(columns)
    widest = max(size for _, size in cuts(tokens // 4, SLOT_SHARES)) * experts
    bf16 = jnp.bfloat16
    hbm = pl.BlockSpec(memory_space=pltpu.HBM)
    dma = pltpu.SemaphoreType.DMA

    def in_hbm(x):
        return pltpu.with_memory_space_constraint(x, pltpu.HBM)

    return pl.pallas_call(
        functools.partial(relay_kernel, sections, experts),
        out_shape=pltpu.VMEM(state.shape, state.dtype),
        in_specs=[hbm] * 6,
        out_specs=pl.BlockSpec(memory_space=pltpu.VMEM),
        scratch_shapes=[
            pltpu.VMEM((width, inner), bf16),
            pltpu.VMEM((hidden_units, width), bf16),
            pltpu.VMEM((1, width), jnp.float32),
            pltpu.VMEM((ticks, top, 1, tokens), jnp.int32),
            pltpu.VMEM((ticks, top, 1, tokens), jnp.float32),
            pltpu.VMEM((ticks, top, 1, tokens), jnp.int32),
            pltpu.VMEM((ticks, top, 1, tokens), jnp.float32),
            pltpu.VMEM((tokens, width), bf16),
            pltpu.VMEM((max(ticks - 1, 1), tokens, width), bf16),
            pltpu.VMEM((ticks, slots + tokens, width), bf16),
            pltpu.VMEM((slots, tokens), bf16),
            pltpu.VMEM((max(ticks - 1, 1), slots, slots + tokens), bf16),
            pltpu.VMEM((ticks, tokens, slots), bf16),
            pltpu.VMEM((ticks, slots, width), bf16),
            pltpu.VMEM((ticks, slots, width), bf16),
            pltpu.VMEM((ticks, slots, width), bf16),
            pltpu.VMEM((widest, inner), jnp.float32),
            dma((4,)),
            dma((chunks,)),
            dma((chunks,)),
            dma((2,)),
            dma((2,)),
            dma,
            dma((ticks, sum(map(len, DISPATCH_RUNS)))),
            dma,
            dma((ticks, sum(map(len, RETURN_RUNS)))),
            dma,
        ],
        compiler_params=pltpu.CompilerParams(
            collective_id=0, has_side_effects=True, vmem_limit_bytes=48 * 2**20
        ),
        name="relay",
    )(
        in_hbm(state),
        in_hbm(norm_gain),
        in_hbm(expert_in),
        in_hbm(expert_out),
        in_hbm(jnp.transpose(route_ids, (0, 3, 1, 2))),
        in_hbm(jnp.transpose(route_weights, (0, 3, 1, 2))),
    )


def solution(mesh):
    in_specs = (
        P("section", "expert", None),
        P("section", None),
        P("section", "expert", None, None),
        P("section", "expert", None, None),
        P(None, "section", "expert", None),
        P(None, "section", "expert", None),
    )
    out_specs = P("section", "expert", None)
    return jax.shard_map(
        functools.partial(on_device, mesh.shape["section"], mesh.shape["expert"]),
        mesh=mesh,
        in_specs=in_specs,
        out_specs=out_specs,
        check_vma=False,
    )
```

```python
import functools

import jax
import jax.numpy as jnp
from jax import lax
from jax.experimental import pallas as pl
from jax.experimental.pallas import tpu as pltpu
from jax.sharding import PartitionSpec as P

epsilon = 1e-06
COLUMN_SHARES = (1, 1, 1, 1)
SLOT_SHARES = (1, 1)
DISPATCH_RUNS = ((1, 1, 1, 1), (2, 1, 1))
RETURN_RUNS = ((2, 2), (1, 1, 1, 1))
MESH = pl.DeviceIdType.MESH


def cuts(total, shares):
    whole = sum(shares)
    ends = [total * sum(shares[: i + 1]) // whole for i in range(len(shares))]
    starts = [0] + ends[:-1]
    return [(a, b - a) for a, b in zip(starts, ends)]


def runs(lengths):
    ends = [sum(lengths[: i + 1]) for i in range(len(lengths))]
    return [(b - n, b) for b, n in zip(ends, lengths)]


def relay_kernel(
    sections,
    experts,
    state_hbm,
    gain_hbm,
    win_hbm,
    wout_hbm,
    ids_hbm,
    wts_hbm,
    out_ref,
    win,
    wout,
    gain,
    ids,
    wts,
    ids_before,
    wts_before,
    state,
    hcur,
    arrive,
    first,
    pick,
    comb,
    sendbuf,
    recvbuf,
    retsend,
    acc,
    load_sem,
    route_ss,
    route_rs,
    disp_ss,
    disp_rs,
    ret_ss,
    ret_rs,
    h_ss,
):
    ticks, top = ids.shape[:2]
    tokens = state.shape[0]
    columns = cuts(state_hbm.shape[2], COLUMN_SHARES)
    width = state_hbm.shape[2]
    chunks = len(columns)
    hidden_units = wout.shape[0]
    capacity = tokens // 4
    slots = experts * capacity
    parts = cuts(capacity, SLOT_SHARES)
    disp_runs = [runs(lengths) for lengths in DISPATCH_RUNS]
    ret_runs = [runs(lengths) for lengths in RETURN_RUNS]

    def disp_sem(p, low):
        return sum(map(len, disp_runs[:p])) + [a for a, _ in disp_runs[p]].index(low)

    def ret_sem(p, low):
        return sum(map(len, ret_runs[:p])) + [a for a, _ in ret_runs[p]].index(low)

    def span(low, high):
        start = columns[low][0]
        return pl.ds(start, sum(columns[high - 1]) - start)

    section = lax.axis_index("section")
    me = lax.axis_index("expert")
    after = lax.rem(section + 1, sections)
    before = lax.rem(section + sections - 1, sections)
    lanes = max(k for k in range(1, experts + 1) if experts % k == 0 and k * k <= experts)
    files = experts // lanes
    steps = [(i, j) for i in range(lanes) for j in range(files)]

    def hops(step):
        i, j = step
        return min(i, lanes - i) + min(j, files - j)

    def peer_at(step):
        i, j = step
        return lax.rem(me // files + i, lanes) * files + lax.rem(lax.rem(me, files) + j, files)

    steps_d = sorted([s for s in steps if s != (0, 0)], key=lambda s: (hops(s), s), reverse=True)
    steps_r = sorted(steps, key=lambda s: (hops(s), s), reverse=True)

    barrier = pltpu.get_barrier_semaphore()
    for step in steps_d:
        pl.semaphore_signal(
            barrier,
            inc=1,
            device_id={"section": section, "expert": peer_at(step)},
            device_id_type=MESH,
        )
    for e in range(experts):
        pl.semaphore_signal(
            barrier, inc=1, device_id={"section": before, "expert": e}, device_id_type=MESH
        )

    load_ids = pltpu.make_async_copy(ids_hbm, ids, load_sem.at[0])
    load_wts = pltpu.make_async_copy(wts_hbm, wts, load_sem.at[1])
    load_gain = pltpu.make_async_copy(gain_hbm, gain, load_sem.at[2])
    load_out = pltpu.make_async_copy(wout_hbm.at[0, 0], wout, load_sem.at[3])

    load_state = pltpu.make_async_copy(state_hbm.at[0], state, load_sem.at[4])
    load_in = pltpu.make_async_copy(win_hbm.at[0, 0], win, load_sem.at[5])

    load_ids.start()
    load_state.start()
    load_wts.start()
    load_gain.start()

    slot_row = lax.broadcasted_iota(jnp.int32, (slots, tokens), 0)
    expert_of = jnp.zeros((slots, tokens), jnp.int32)
    slot_of = slot_row
    for low, half in parts:
        for e in range(experts):
            start = low * experts + e * half
            inside = slot_row >= start
            expert_of = jnp.where(inside, e, expert_of)
            slot_of = jnp.where(inside, slot_row - start + low, slot_of)
    slot_of = slot_of.astype(jnp.float32)
    row_i = lax.broadcasted_iota(jnp.int32, (tokens, tokens), 0)
    col_i = lax.broadcasted_iota(jnp.int32, (tokens, tokens), 1)
    earlier = jnp.where(row_i < col_i, 1.0, 0.0).astype(jnp.bfloat16)

    def kept_slots(ids_ref, t):
        hit = jnp.zeros((slots, tokens), jnp.float32)
        for k in range(top):
            hit = jnp.where(ids_ref[t, k] == expert_of, 1.0, hit)
        rank = jnp.dot(hit.astype(jnp.bfloat16), earlier, preferred_element_type=jnp.float32)
        return jnp.where(rank == slot_of, hit, 0.0)

    def make_comb(t):
        mix = jnp.zeros((slots, tokens), jnp.float32)
        for k in range(top):
            mix = jnp.where(ids_before[t, k] == expert_of, wts_before[t, k], mix)
        weighted = kept_slots(ids_before, t) * mix
        comb[t] = jnp.transpose(weighted).astype(jnp.bfloat16)

    def make_pick(t):
        keep = kept_slots(ids, t).astype(jnp.bfloat16)
        mixed = jnp.dot(keep, comb[t - 1], preferred_element_type=jnp.float32)
        pick[t - 1, :, pl.ds(0, slots)] = mixed.astype(jnp.bfloat16)
        pick[t - 1, :, pl.ds(slots, tokens)] = keep

    def route_copies():
        return [
            pltpu.make_async_remote_copy(
                src_ref=mine,
                dst_ref=theirs,
                send_sem=route_ss.at[i],
                recv_sem=route_rs.at[i],
                device_id={"section": after, "expert": me},
                device_id_type=MESH,
            )
            for i, (mine, theirs) in enumerate(((ids, ids_before), (wts, wts_before)))
        ]

    def h_copy(t, c):
        cols = pl.ds(*columns[c])
        return pltpu.make_async_remote_copy(
            src_ref=state.at[:, cols] if t == 0 else hcur.at[t - 1, :, cols],
            dst_ref=arrive.at[t, pl.ds(slots, tokens), cols],
            send_sem=h_ss,
            recv_sem=ret_rs.at[t, ret_sem(len(parts) - 1, c)],
            device_id={"section": after, "expert": me},
            device_id_type=MESH,
        )

    def part_rows(p, e):
        low, half = parts[p]
        return pl.ds(pl.multiple_of(low * experts + e * half, 8), half)

    def part_all(p):
        low, half = parts[p]
        return pl.ds(low * experts, half * experts)

    def send_rows(t, p, low, high):
        for step in steps_d:
            peer = peer_at(step)
            pltpu.make_async_remote_copy(
                src_ref=sendbuf.at[t, part_rows(p, peer), span(low, high)],
                dst_ref=recvbuf.at[t, part_rows(p, me), span(low, high)],
                send_sem=disp_ss,
                recv_sem=disp_rs.at[t, disp_sem(p, low)],
                device_id={"section": section, "expert": peer},
                device_id_type=MESH,
            ).start()

    def await_rows(t, p, c):
        first_row, half = parts[p]
        for low, high in disp_runs[p]:
            if low == c:
                block = recvbuf.at[
                    t, pl.ds(first_row * experts, (experts - 1) * half), span(low, high)
                ]
                pltpu.make_async_remote_copy(
                    src_ref=block,
                    dst_ref=block,
                    send_sem=disp_ss,
                    recv_sem=disp_rs.at[t, disp_sem(p, low)],
                    device_id={"section": section, "expert": lax.rem(me + 1, experts)},
                    device_id_type=MESH,
                ).wait_recv()

    def send_served(t, p, c):
        for low, high in ret_runs[p]:
            if high == c + 1:
                for step in steps_r:
                    peer = peer_at(step)
                    pltpu.make_async_remote_copy(
                        src_ref=retsend.at[t, part_rows(p, peer), span(low, high)],
                        dst_ref=arrive.at[t, part_rows(p, me), span(low, high)],
                        send_sem=ret_ss,
                        recv_sem=ret_rs.at[t, ret_sem(p, low)],
                        device_id={"section": after, "expert": peer},
                        device_id_type=MESH,
                    ).start()

    def await_served(t, c):
        last = len(parts) - 1
        for p in range(len(parts)):
            for low, high in ret_runs[p]:
                if low == c:
                    rows = part_all(p)
                    if p == last:
                        rows = pl.ds(rows.start, rows.size + tokens)
                    block = arrive.at[t, rows, span(low, high)]
                    pltpu.make_async_remote_copy(
                        src_ref=block,
                        dst_ref=block,
                        send_sem=ret_ss,
                        recv_sem=ret_rs.at[t, ret_sem(p, low)],
                        device_id={"section": before, "expert": me},
                        device_id_type=MESH,
                    ).wait_recv()

    def fill(t, c, picker, source):
        rows = jnp.dot(picker, source, preferred_element_type=jnp.float32)
        sendbuf[t, :, pl.ds(*columns[c])] = rows.astype(jnp.bfloat16)

    def keep_own(t, c):
        cols = pl.ds(*columns[c])
        for p in range(len(parts)):
            own = part_rows(p, me)
            recvbuf[t, own, cols] = sendbuf[t, own, cols]

    def dispatch(t, c):
        for low, high in disp_runs[0]:
            if high == c + 1:
                send_rows(t, 0, low, high)
        if c == chunks - 1:
            for p in range(1, len(parts)):
                for low, high in disp_runs[p]:
                    send_rows(t, p, low, high)

    load_ids.wait()
    first[...] = kept_slots(ids, 0).astype(jnp.bfloat16)
    load_state.wait()
    load_in.start()
    load_out.start()
    for c in range(chunks):
        fill(0, c, first[...], state[:, pl.ds(*columns[c])])
        keep_own(0, c)
    load_wts.wait()
    pl.semaphore_wait(barrier, experts - 1 + experts)
    for c in range(chunks):
        dispatch(0, c)
    for copy in route_copies():
        copy.start()
    for c in range(chunks):
        h_copy(0, c).start()
    for copy in route_copies():
        copy.wait_recv()
    for t in range(ticks):
        make_comb(t)
    for t in range(1, ticks):
        make_pick(t)

    load_gain.wait()
    for t in range(ticks):
        for p in range(len(parts)):
            rows = part_all(p)
            group = rows.size
            squares = jnp.zeros((group, 1), jnp.float32)
            for c in range(chunks):
                cols = pl.ds(*columns[c])
                if t == 0 and p == 0 and c == 0:
                    load_in.wait()
                await_rows(t, p, c)
                wide = recvbuf[t, rows, cols].astype(jnp.float32)
                squares = squares + jnp.sum(wide * wide, axis=-1, keepdims=True)
                scaled = (wide * gain[:, cols]).astype(jnp.bfloat16)
                part = jnp.dot(scaled, win[cols, :], preferred_element_type=jnp.float32)
                if c == 0:
                    acc[pl.ds(0, group), :] = part
                else:
                    acc[pl.ds(0, group), :] += part
            rescale = lax.rsqrt(squares / width + epsilon)
            gate = acc[pl.ds(0, group), :hidden_units] * rescale
            up = acc[pl.ds(0, group), hidden_units:] * rescale
            activated = (gate / (1.0 + jnp.exp(-gate)) * up).astype(jnp.bfloat16)
            if t == 0 and p == 0:
                load_out.wait()
            for c in range(chunks):
                served = jnp.dot(
                    activated, wout[:, pl.ds(*columns[c])], preferred_element_type=jnp.float32
                )
                retsend[t, rows, pl.ds(*columns[c])] = served.astype(jnp.bfloat16)
                send_served(t, p, c)
        for c in range(chunks):
            cols = pl.ds(*columns[c])
            await_served(t, c)
            if t < ticks - 1:
                fill(t + 1, c, pick[t], arrive[t, :, cols])
                dispatch(t + 1, c)
            branch = jnp.dot(
                comb[t], arrive[t, pl.ds(0, slots), cols], preferred_element_type=jnp.float32
            )
            stay = arrive[t, pl.ds(slots, tokens), cols].astype(jnp.float32)
            fresh = (stay + branch).astype(jnp.bfloat16)
            if t == ticks - 1:
                out_ref[0, :, cols] = fresh
            else:
                hcur[t, :, cols] = fresh
                h_copy(t + 1, c).start()
                keep_own(t + 1, c)

    for copy in route_copies():
        copy.wait_send()
    for sent, sem in (
        (sendbuf.at[:, pl.ds(0, slots - capacity)], disp_ss),
        (retsend, ret_ss),
        (arrive.at[:, pl.ds(slots, tokens)], h_ss),
    ):
        pltpu.make_async_remote_copy(
            src_ref=sent,
            dst_ref=sent,
            send_sem=sem,
            recv_sem=disp_rs.at[0, 0],
            device_id={"section": after, "expert": me},
            device_id_type=MESH,
        ).wait_send()


def on_device(sections, experts, state, norm_gain, expert_in, expert_out, route_ids, route_weights):
    ticks, _, _, top = route_ids.shape
    tokens, width = state.shape[1:]
    inner = expert_in.shape[3]
    hidden_units = expert_out.shape[2]
    slots = experts * (tokens // 4)
    columns = cuts(width, COLUMN_SHARES)
    widest = max(size for _, size in cuts(tokens // 4, SLOT_SHARES)) * experts
    bf16 = jnp.bfloat16
    hbm = pl.BlockSpec(memory_space=pltpu.HBM)
    dma = pltpu.SemaphoreType.DMA

    def in_hbm(x):
        return pltpu.with_memory_space_constraint(x, pltpu.HBM)

    return pl.pallas_call(
        functools.partial(relay_kernel, sections, experts),
        out_shape=pltpu.VMEM(state.shape, state.dtype),
        in_specs=[hbm] * 6,
        out_specs=pl.BlockSpec(memory_space=pltpu.VMEM),
        scratch_shapes=[
            pltpu.VMEM((width, inner), bf16),
            pltpu.VMEM((hidden_units, width), bf16),
            pltpu.VMEM((1, width), jnp.float32),
            pltpu.VMEM((ticks, top, 1, tokens), jnp.int32),
            pltpu.VMEM((ticks, top, 1, tokens), jnp.float32),
            pltpu.VMEM((ticks, top, 1, tokens), jnp.int32),
            pltpu.VMEM((ticks, top, 1, tokens), jnp.float32),
            pltpu.VMEM((tokens, width), bf16),
            pltpu.VMEM((max(ticks - 1, 1), tokens, width), bf16),
            pltpu.VMEM((ticks, slots + tokens, width), bf16),
            pltpu.VMEM((slots, tokens), bf16),
            pltpu.VMEM((max(ticks - 1, 1), slots, slots + tokens), bf16),
            pltpu.VMEM((ticks, tokens, slots), bf16),
            pltpu.VMEM((ticks, slots, width), bf16),
            pltpu.VMEM((ticks, slots, width), bf16),
            pltpu.VMEM((ticks, slots, width), bf16),
            pltpu.VMEM((widest, inner), jnp.float32),
            dma((6,)),
            dma((2,)),
            dma((2,)),
            dma,
            dma((ticks, sum(map(len, DISPATCH_RUNS)))),
            dma,
            dma((ticks, sum(map(len, RETURN_RUNS)))),
            dma,
        ],
        compiler_params=pltpu.CompilerParams(
            collective_id=0, has_side_effects=True, vmem_limit_bytes=48 * 2**20
        ),
        name="relay",
    )(
        in_hbm(state),
        in_hbm(norm_gain),
        in_hbm(expert_in),
        in_hbm(expert_out),
        in_hbm(jnp.transpose(route_ids, (0, 3, 1, 2))),
        in_hbm(jnp.transpose(route_weights, (0, 3, 1, 2))),
    )


def solution(mesh):
    in_specs = (
        P("section", "expert", None),
        P("section", None),
        P("section", "expert", None, None),
        P("section", "expert", None, None),
        P(None, "section", "expert", None),
        P(None, "section", "expert", None),
    )
    out_specs = P("section", "expert", None)
    return jax.shard_map(
        functools.partial(on_device, mesh.shape["section"], mesh.shape["expert"]),
        mesh=mesh,
        in_specs=in_specs,
        out_specs=out_specs,
        check_vma=False,
    )
```
